128 devices in a mesh: section: 2 (over core), node: 16 (over x, z), local: 4 (over y).
Axes of the slice: x: 4, y: 4, z: 4, core: 2. Of those that a mesh axis runs over, the one named last changes fastest.
Arguments:
- tokens: bfloat16 [2, 4096, 768], P(None, ('node', 'local')), may hold values from -18 to 18
- expert_ids: int32 [2, 2, 4096, 2], P('section', None, ('node', 'local')), may hold values from 0 to 63, as said below
- slots: int32 [2, 2, 4096, 2], P('section', None, ('node', 'local')), may hold values from -1 to 7, as said below
- gates: float32 [2, 2, 4096, 2], P('section', None, ('node', 'local')), may hold values from 0.2 to 1
- gain: float32 [2, 768], P('section'), may hold values from 0.5 to 1.5
- w_gate: bfloat16 [2, 64, 768, 3072], P('section', ('node', 'local')), may hold values from -0.21875 to 0.21875
- w_up: bfloat16 [2, 64, 768, 3072], P('section', ('node', 'local')), may hold values from -0.21875 to 0.21875
- w_down: bfloat16 [2, 64, 3072, 768], P('section', ('node', 'local')), may hold values from -0.109375 to 0.109375
Outputs:
- hidden: bfloat16 [2, 2, 4096, 768], P('section', None, ('node', 'local'))
The draws below stay inside these ranges and needn't reach their ends.
Inputs may be any that keep to these rules, and one draw needn't show every extreme that they name: `expert_ids`: in each layer and micro-batch the two ids of a token differ, no expert is named by more than 256 tokens, and some expert is named by exactly 256. Expert e lies on node e // 4. Among one device's 64 tokens of a micro-batch and layer, the kept tokens that reach one node hold distinct slots below 8, and the two choices of a token on one node carry the same slot; -1 marks a dropped choice.
All inputs are finite; a program needn't handle non-finite values.
Results may differ from the reference program's by a relative error of at most 0.0085.
Values may be sent and summed in bfloat16 or wider, within the bound.
No kernel may reach another device: no remote copies, remote signals or barrier semaphores. Data moves between devices by JAX's collectives and lax.ppermute only.
A program may use at most 64 MiB of HBM per device.

```python
import math
import jax
import jax.numpy as jnp
from jax import lax

D = 768
FF = 3072
TOP = 2
TOK_MB = 64
MICRO = 2
LAYERS = 2
EXPERTS = 64
TOKENS = 4096
CAP = 8
ECAP = 256
N_NODE = 16
N_LOCAL = 4


def one_group(group_key):
    subkeys = jax.random.split(group_key, 5)
    node_order = jax.random.permutation(subkeys[0], N_NODE)
    local_order = jax.random.permutation(subkeys[1], N_LOCAL)
    second_node_order = jax.random.permutation(subkeys[4], N_NODE)
    half_count = EXPERTS // 2
    quarter = EXPERTS // 4
    half_local = N_LOCAL // 2
    mean_load = 2 * TOK_MB
    rank_ids = jnp.arange(half_count, dtype=jnp.int32)
    upper_gain = mean_load * (quarter - rank_ids) // quarter
    lower_gain = mean_load * (quarter - (half_count - 1 - rank_ids)) // quarter
    quotas = jnp.where(rank_ids < quarter, mean_load + upper_gain, mean_load - lower_gain)
    bounds = jnp.cumsum(quotas)
    places = jnp.arange(TOKENS, dtype=jnp.int32)
    which_rank = jnp.sum((places[:, None] >= bounds[None, :]).astype(jnp.int32), axis=1)
    first_node = node_order[which_rank // half_local]
    second_node = second_node_order[which_rank // half_local]
    first_ids = first_node * N_LOCAL + local_order[which_rank % half_local]
    second = second_node * N_LOCAL + local_order[half_local + which_rank % half_local]
    first_ids = first_ids[jax.random.permutation(subkeys[2], TOKENS)]
    second = second[jax.random.permutation(subkeys[3], TOKENS)]
    routing = jnp.stack([first_ids, second], axis=1).astype(jnp.int32)
    device_route = routing.reshape(N_NODE * N_LOCAL, TOK_MB, 2)
    node_route = device_route // N_LOCAL
    node_span = jnp.arange(N_NODE, dtype=jnp.int32)
    touched = ((node_route[..., 0:1] == node_span) | (node_route[..., 1:2] == node_span)).astype(jnp.int32)
    before = jnp.cumsum(touched, axis=1) - touched
    slot_pick = jnp.take_along_axis(before, node_route, axis=2)
    slot_vals = jnp.where(slot_pick < CAP, slot_pick, -1).reshape(TOKENS, 2).astype(jnp.int32)
    return (routing, slot_vals)


def route_tables(key):
    base_key = jax.random.fold_in(key, 7)
    group_keys = jax.random.split(base_key, LAYERS * MICRO)
    expert_table, slot_table = jax.vmap(one_group)(group_keys)
    return (expert_table.reshape(LAYERS, MICRO, TOKENS, 2), slot_table.reshape(LAYERS, MICRO, TOKENS, 2))


def draw_expert_ids(key, part):
    return route_tables(key)[0]


def draw_slots(key, part):
    return route_tables(key)[1]


def draw_tokens(key, part):
    subkeys = jax.random.split(jax.random.fold_in(key, 3), 2)
    values = jnp.clip(jax.random.normal(subkeys[0], (MICRO, TOKENS, D), jnp.float32), -6.0, 6.0)
    scales = jnp.exp(jax.random.uniform(subkeys[1], (MICRO, TOKENS, 1), jnp.float32, math.log(0.5), math.log(2.0)))
    return (values * scales).astype(jnp.bfloat16)


def steps_of(key, shape, cuts, low, high):
    level = 1.0
    for dim, shards_of in cuts:
        draws = jax.random.uniform(jax.random.fold_in(jax.random.fold_in(key, 6), dim), (shards_of,), jnp.float32, low / len(cuts), high / len(cuts))
        level = level * jnp.repeat(jnp.exp(draws), shape[dim] // shards_of).reshape((-1,) + (1,) * (len(shape) - 1 - dim))
    return level


def centred(own_key, dims, deviation, most, pieces=(), kind=jnp.bfloat16):
    result = jax.random.normal(own_key, dims, jnp.float32) * deviation
    if len(pieces) > 0:
        result = steps_of(own_key, dims, pieces, -0.22, 0.18) * result
    return jnp.clip(result, min=-most, max=most).astype(kind)


def setup_inputs(seed: int = 0) -> dict:
    key_list = jax.random.split(jax.random.key(seed), 9)
    tokens = draw_tokens(jax.random.fold_in(key_list[8], 71), 0)
    expert_ids = draw_expert_ids(jax.random.fold_in(key_list[8], 71), 0)
    slots = draw_slots(jax.random.fold_in(key_list[8], 71), 0)
    gates = jnp.clip(0.2 + 0.8 * jax.random.uniform(key_list[3], (LAYERS, MICRO, TOKENS, TOP), jnp.float32) ** steps_of(key_list[3], (LAYERS, MICRO, TOKENS, TOP), ((0, 2), (2, 64)), -0.2, 0.2), 0.2, 1.0)
    gain = jnp.clip(1.0 + 0.1 * jax.random.normal(key_list[4], (LAYERS, D), jnp.float32), 0.5, 1.5)
    w_gate = centred(key_list[5], (LAYERS, EXPERTS, D, FF), D ** -0.5, 0.21875, ((0, 2), (1, 64)))
    w_up = centred(key_list[6], (LAYERS, EXPERTS, D, FF), D ** -0.5, 0.21875, ((0, 2), (1, 64)))
    w_down = centred(key_list[7], (LAYERS, EXPERTS, FF, D), FF ** -0.5, 0.109375, ((0, 2), (1, 64)))
    return {"tokens": tokens, "expert_ids": expert_ids, "slots": slots, "gates": gates, "gain": gain, "w_gate": w_gate, "w_up": w_up, "w_down": w_down}


def rms_normed(values, gain_row):
    floats = values.astype(jnp.float32)
    mean_square = lax.optimization_barrier(jnp.mean(floats * floats, axis=-1, keepdims=True))
    return (floats * lax.rsqrt(mean_square + 1e-05) * gain_row).astype(jnp.bfloat16)

def expert_apply(picked, gate_mat, up_mat, down_mat):
    gate_act = jnp.dot(picked, gate_mat, preferred_element_type=jnp.float32)
    up_act = jnp.dot(picked, up_mat, preferred_element_type=jnp.float32)
    inner = (jax.nn.gelu(gate_act, approximate=True) * up_act).astype(jnp.bfloat16)
    return jnp.dot(inner, down_mat, preferred_element_type=jnp.float32)

def moe_layer(layer_in, routing, slot_ids, gate_vals, gain_row, gate_all, up_all, down_all):
    normed = rms_normed(layer_in, gain_row)
    keep_weight = jnp.where(slot_ids >= 0, gate_vals, jnp.float32(0.0)).astype(jnp.float32)

    def per_expert(totals, expert):
        hit_mask = routing == expert
        any_hit = jnp.any(hit_mask, axis=1)
        row_index = jnp.nonzero(any_hit, size=ECAP, fill_value=0)[0].astype(jnp.int32)
        valid_rows = jnp.arange(ECAP, dtype=jnp.int32) < jnp.sum(any_hit.astype(jnp.int32))
        picked = normed[row_index]
        outputs = expert_apply(picked, gate_all[expert], up_all[expert], down_all[expert])
        row_weight = lax.optimization_barrier(jnp.sum(jnp.where(hit_mask, keep_weight, jnp.float32(0.0)), axis=1))[row_index]
        row_weight = jnp.where(valid_rows, row_weight, jnp.float32(0.0))
        scaled = lax.optimization_barrier((row_weight[:, None] * outputs).astype(jnp.bfloat16)).astype(jnp.float32)
        choice_mask = (hit_mask[row_index] & valid_rows[:, None]).astype(jnp.float32)
        totals = totals.at[row_index].add(scaled[:, None, :] * choice_mask[:, :, None])
        return (totals, None)
    start = jnp.zeros((layer_in.shape[0], 2, layer_in.shape[1]), jnp.float32)
    totals, _ = lax.scan(per_expert, start, jnp.arange(EXPERTS, dtype=jnp.int32))
    same_node = routing[:, 0] // N_LOCAL == routing[:, 1] // N_LOCAL
    pair_sum = totals[:, 0] + totals[:, 1]
    together = lax.optimization_barrier(pair_sum.astype(jnp.bfloat16)).astype(jnp.float32)
    mixed_rows = jnp.where(same_node[:, None], together, pair_sum)
    return (layer_in.astype(jnp.float32) + mixed_rows).astype(jnp.bfloat16)

def reference(tokens, expert_ids, slots, gates, gain, w_gate, w_up, w_down):
    current = [tokens[batch_index] for batch_index in range(MICRO)]
    stacked = []
    for layer_index in range(LAYERS):
        produced = []
        for batch_index in range(MICRO):
            produced.append(moe_layer(current[batch_index], expert_ids[layer_index, batch_index], slots[layer_index, batch_index], gates[layer_index, batch_index], gain[layer_index], w_gate[layer_index], w_up[layer_index], w_down[layer_index]))
        stacked.append(jnp.stack(produced))
        current = produced
    return jnp.stack(stacked)
```

```python
import functools
import math

import jax
import jax.numpy as jnp
from jax import lax
from jax.experimental import pallas as pl
from jax.experimental.pallas import tpu as pltpu
from jax.sharding import PartitionSpec as P

CAP = 8
ECAP = 256
F32 = jnp.float32
BF16 = jnp.bfloat16
VMEM = pl.BlockSpec(memory_space=pltpu.VMEM)
SMEM = pl.BlockSpec(memory_space=pltpu.SMEM)
ANY = pl.BlockSpec(memory_space=pl.ANY)


def normed_rows(h, gain):
    x = h.astype(F32)
    ms = jnp.mean(x * x, axis=-1, keepdims=True)
    return (x * lax.rsqrt(ms + 1e-05) * gain).astype(BF16)


def pick(sec, layer, own_ref, oth_ref):
    return jnp.where(sec == layer, own_ref[sec], oth_ref[sec])


def pack_rows(normed, meta, slots):
    tok = normed.shape[0]
    pos = meta[0:2].astype(jnp.int32)
    span = lax.broadcasted_iota(jnp.int32, (slots, tok), 0)
    hit = (span == pos[0:1]) | (span == pos[1:2])
    onehot = jnp.where(hit, 1.0, 0.0).astype(BF16)
    return jnp.dot(onehot, normed, preferred_element_type=F32).astype(BF16)


def mix_rows(h, ret, meta):
    tok = h.shape[0]
    slots = ret.shape[0]
    span = lax.broadcasted_iota(jnp.int32, (tok, slots), 1)
    pos = meta[:, 0:2].astype(jnp.int32)
    comb = jnp.where(span == pos[:, 0:1], meta[:, 2:3], 0.0)
    comb = comb + jnp.where(span == pos[:, 1:2], meta[:, 3:4], 0.0)
    high = comb.astype(BF16)
    low = (comb - high.astype(F32)).astype(BF16)
    mixed = jnp.dot(high, ret, preferred_element_type=F32)
    mixed = mixed + jnp.dot(low, ret, preferred_element_type=F32)
    return (h.astype(F32) + mixed).astype(BF16)


def first_kernel(sec_ref, tok_ref, own_ref, oth_ref, gown_ref, goth_ref, out_ref):
    sec = sec_ref[0]
    gain = jnp.where(sec == 0, gown_ref[...], goth_ref[...])
    meta = pick(sec, 0, own_ref, oth_ref)
    out_ref[...] = pack_rows(normed_rows(tok_ref[sec], gain), meta, out_ref.shape[0])


def middle_kernel(sec_ref, tok_ref, ret_ref, cown_ref, coth_ref, own_ref, oth_ref, gown_ref, goth_ref, h_ref, out_ref):
    sec = sec_ref[0]
    h = mix_rows(tok_ref[sec], ret_ref[...], pick(sec, 0, cown_ref, coth_ref))
    h_ref[...] = h
    gain = jnp.where(sec == 1, gown_ref[...], goth_ref[...])
    meta = pick(sec, 1, own_ref, oth_ref)
    out_ref[...] = pack_rows(normed_rows(h, gain), meta, out_ref.shape[0])


def last_kernel(sec_ref, h_ref, ret_ref, cown_ref, coth_ref, keep_ref, send_ref):
    sec = sec_ref[0]
    h0 = h_ref[...]
    h1 = mix_rows(h0, ret_ref[...], pick(sec, 1, cown_ref, coth_ref))
    keep_ref[...] = jnp.where(sec == 0, h0, h1)
    send_ref[...] = jnp.where(sec == 0, h1, h0)


def expert_kernel(layer, tile, sec_ref, x_ref, go_ref, uo_ref, do_ref, gp_ref, up_ref, dp_ref, out_ref,
                  gbuf, ubuf, dbuf, sems):
    sec = sec_ref[0]
    width = x_ref.shape[1]
    slots = x_ref.shape[0]
    steps = gbuf.shape[0]

    def copies(g, u, d, k):
        cols = pl.ds(k * tile, tile)
        return (
            pltpu.make_async_copy(g.at[0, 0, :, cols], gbuf.at[k], sems.at[0, k]),
            pltpu.make_async_copy(u.at[0, 0, :, cols], ubuf.at[k], sems.at[1, k]),
            pltpu.make_async_copy(d.at[0, 0, cols, :], dbuf.at[k], sems.at[2, k]),
        )

    @pl.when(sec == layer)
    def _():
        for k in range(steps):
            for c in copies(go_ref, uo_ref, do_ref, k):
                c.start()

    @pl.when(sec != layer)
    def _():
        for k in range(steps):
            for c in copies(gp_ref, up_ref, dp_ref, k):
                c.start()

    x = x_ref[...]
    some = jnp.where(x != 0, 1.0, 0.0).astype(BF16)
    ones = jnp.ones((8, width), BF16)
    count = lax.dot_general(ones, some, (((1,), (1,)), ((), ())), preferred_element_type=F32)
    valid = count > 0.0
    before = lax.broadcasted_iota(jnp.int32, (slots, slots), 0) < lax.broadcasted_iota(jnp.int32, (slots, slots), 1)
    upper = jnp.where(before, 1.0, 0.0).astype(BF16)
    rank = jnp.dot(jnp.where(valid, 1.0, 0.0).astype(BF16), upper, preferred_element_type=F32)
    rank = jnp.where(valid, rank, -1.0).astype(jnp.int32)
    rows = lax.broadcasted_iota(jnp.int32, (ECAP, slots), 0)
    choose = jnp.where(rows == rank[0:1], 1.0, 0.0).astype(BF16)
    picked = jnp.dot(choose, x, preferred_element_type=F32).astype(BF16)

    acc = jnp.zeros((ECAP, width), F32)
    for k in range(steps):
        cg, cu, cd = copies(go_ref, uo_ref, do_ref, k)
        cg.wait()
        gate = jnp.dot(picked, gbuf[k], preferred_element_type=F32)
        cu.wait()
        up = jnp.dot(picked, ubuf[k], preferred_element_type=F32)
        inner = (jax.nn.gelu(gate, approximate=True) * up).astype(BF16)
        cd.wait()
        acc = acc + jnp.dot(inner, dbuf[k], preferred_element_type=F32)
    out_ref[...] = lax.dot_general(
        choose, acc.astype(BF16), (((0,), (0,)), ((), ())), preferred_element_type=F32
    ).astype(BF16)


def expert(layer, sec, arrived, own, other):
    slots, width = arrived.shape
    hidden = own[0].shape[-1]
    tile = 512
    steps = hidden // tile
    return pl.pallas_call(
        functools.partial(expert_kernel, layer, tile),
        out_shape=jax.ShapeDtypeStruct((slots, width), BF16),
        in_specs=[SMEM, VMEM] + [ANY] * 6,
        out_specs=VMEM,
        scratch_shapes=[
            pltpu.VMEM((steps, width, tile), BF16),
            pltpu.VMEM((steps, width, tile), BF16),
            pltpu.VMEM((steps, tile, width), BF16),
            pltpu.SemaphoreType.DMA((3, steps)),
        ],
        name="expert%d" % layer,
    )(sec, arrived, *own, *other)


def small(kernel, outs, *args, name):
    return pl.pallas_call(
        kernel,
        out_shape=[jax.ShapeDtypeStruct(s, BF16) for s in outs],
        in_specs=[SMEM] + [VMEM] * (len(args) - 1),
        out_specs=[VMEM] * len(outs),
        name=name,
    )(*args)


def on_device(tokens, expert_ids, slots, gates, gain, w_gate, w_up, w_down):
    tok, width = tokens.shape[1:]
    count = lax.axis_size("node") * lax.axis_size("local")
    rows = count * CAP
    swap = [(0, 1), (1, 0)]
    axes = ("node", "local")
    sec = lax.axis_index("section").astype(jnp.int32).reshape(1)

    ids = expert_ids[0].transpose(0, 2, 1)
    slot = slots[0].transpose(0, 2, 1)
    pos = jnp.where(slot >= 0, ids * CAP + slot, -1).astype(F32)
    meta = jnp.concatenate([pos, gates[0].transpose(0, 2, 1)], axis=1)
    meta_p = lax.ppermute(meta, "section", swap)
    gain_p = lax.ppermute(gain, "section", swap)
    own = (w_gate, w_up, w_down)
    other = tuple(lax.ppermute(w, "section", swap) for w in own)
    cols = meta.transpose(0, 2, 1)
    cols_p = meta_p.transpose(0, 2, 1)

    def exchange(x):
        x = x.reshape(count, CAP, width)
        return lax.all_to_all(x, axes, split_axis=0, concat_axis=0, tiled=True).reshape(rows, width)

    (packed,) = small(first_kernel, [(rows, width)], sec, tokens, meta, meta_p, gain, gain_p, name="first")
    back = exchange(expert(0, sec, exchange(packed), own, other))
    h0, packed = small(middle_kernel, [(tok, width), (rows, width)], sec, tokens, back, cols, cols_p,
                       meta, meta_p, gain, gain_p, name="middle")
    back = exchange(expert(1, sec, exchange(packed), own, other))
    keep, send = small(last_kernel, [(tok, width), (tok, width)], sec, h0, back, cols, cols_p, name="last")
    got = lax.ppermute(send, "section", swap)
    first = sec[0] == 0
    return jnp.stack([jnp.where(first, keep, got), jnp.where(first, got, keep)])[None]


def solution(mesh):
    placed = (
        P(None, ("node", "local"), None),
        P("section", None, ("node", "local"), None),
        P("section", None, ("node", "local"), None),
        P("section", None, ("node", "local"), None),
        P("section", None),
        P("section", ("node", "local"), None, None),
        P("section", ("node", "local"), None, None),
        P("section", ("node", "local"), None, None),
    )
    return jax.shard_map(
        on_device,
        mesh=mesh,
        in_specs=placed,
        out_specs=P("section", None, ("node", "local"), None),
        check_vma=False,
    )
```

```python
import functools
import math

import jax
import jax.numpy as jnp
from jax import lax
from jax.experimental import pallas as pl
from jax.experimental.pallas import tpu as pltpu
from jax.sharding import PartitionSpec as P

CAP = 8
ECAP = 256
F32 = jnp.float32
BF16 = jnp.bfloat16
VMEM = pl.BlockSpec(memory_space=pltpu.VMEM)
SMEM = pl.BlockSpec(memory_space=pltpu.SMEM)
ANY = pl.BlockSpec(memory_space=pl.ANY)


def normed_rows(h, gain):
    x = h.astype(F32)
    ms = jnp.mean(x * x, axis=-1, keepdims=True)
    return (x * lax.rsqrt(ms + 1e-05) * gain).astype(BF16)


def pick(sec, layer, own_ref, oth_ref):
    return jnp.where(sec == layer, own_ref[0, sec], oth_ref[0, sec])


def places(sec, layer, ids_ref, idp_ref, slot_ref, slotp_ref):
    slot = pick(sec, layer, slot_ref, slotp_ref)
    return jnp.where(slot >= 0, pick(sec, layer, ids_ref, idp_ref) * CAP + slot, -1)


def pack_rows(normed, pos, slots):
    span = lax.broadcasted_iota(jnp.int32, (slots, normed.shape[0]), 0)
    hit = (span == pos[0:1]) | (span == pos[1:2])
    onehot = jnp.where(hit, 1.0, 0.0).astype(BF16)
    return jnp.dot(onehot, normed, preferred_element_type=F32).astype(BF16)


def mix_rows(h, ret, pos, weight):
    span = lax.broadcasted_iota(jnp.int32, (ret.shape[0], h.shape[0]), 0)
    comb = jnp.where(span == pos[0:1], weight[0:1], 0.0) + jnp.where(span == pos[1:2], weight[1:2], 0.0)
    high = comb.astype(BF16)
    low = (comb - high.astype(F32)).astype(BF16)
    down = (((0,), (0,)), ((), ()))
    mixed = lax.dot_general(high, ret, down, preferred_element_type=F32)
    mixed = mixed + lax.dot_general(low, ret, down, preferred_element_type=F32)
    return (h.astype(F32) + mixed).astype(BF16)


def first_kernel(sec_ref, tok_ref, ids_ref, idp_ref, slot_ref, slotp_ref, gown_ref, goth_ref, out_ref):
    sec = sec_ref[0]
    gain = jnp.where(sec == 0, gown_ref[...], goth_ref[...])
    pos = places(sec, 0, ids_ref, idp_ref, slot_ref, slotp_ref)
    out_ref[...] = pack_rows(normed_rows(tok_ref[sec], gain), pos, out_ref.shape[0])


def middle_kernel(sec_ref, tok_ref, ret_ref, ids_ref, idp_ref, slot_ref, slotp_ref, gown_ref, goth_ref,
                  wown_ref, woth_ref, h_ref, out_ref):
    sec = sec_ref[0]
    pos = places(sec, 0, ids_ref, idp_ref, slot_ref, slotp_ref)
    h = mix_rows(tok_ref[sec], ret_ref[...], pos, pick(sec, 0, wown_ref, woth_ref))
    h_ref[...] = h
    gain = jnp.where(sec == 1, gown_ref[...], goth_ref[...])
    pos = places(sec, 1, ids_ref, idp_ref, slot_ref, slotp_ref)
    out_ref[...] = pack_rows(normed_rows(h, gain), pos, out_ref.shape[0])


def last_kernel(sec_ref, h_ref, ret_ref, ids_ref, idp_ref, slot_ref, slotp_ref, wown_ref, woth_ref, keep_ref, send_ref):
    sec = sec_ref[0]
    h0 = h_ref[...]
    pos = places(sec, 1, ids_ref, idp_ref, slot_ref, slotp_ref)
    h1 = mix_rows(h0, ret_ref[...], pos, pick(sec, 1, wown_ref, woth_ref))
    keep_ref[...] = jnp.where(sec == 0, h0, h1)
    send_ref[...] = jnp.where(sec == 0, h1, h0)


def expert_kernel(layer, tile, ahead, sec_ref, x_ref, go_ref, uo_ref, do_ref, gp_ref, up_ref, dp_ref, out_ref,
                  gbuf, ubuf, dbuf, sems):
    sec = sec_ref[0]
    slots, width = x_ref.shape
    steps = gbuf.shape[0]

    def copies(g, u, d, k):
        cols = pl.ds(k * tile, tile)
        return (
            pltpu.make_async_copy(g.at[0, 0, :, cols], gbuf.at[k], sems.at[0, k]),
            pltpu.make_async_copy(u.at[0, 0, :, cols], ubuf.at[k], sems.at[1, k]),
            pltpu.make_async_copy(d.at[0, 0, cols, :], dbuf.at[k], sems.at[2, k]),
        )

    def fetch(k):
        @pl.when(sec == layer)
        def _():
            for c in copies(go_ref, uo_ref, do_ref, k):
                c.start()

        @pl.when(sec != layer)
        def _():
            for c in copies(gp_ref, up_ref, dp_ref, k):
                c.start()

    for k in range(ahead):
        fetch(k)
    x = x_ref[...]
    some = jnp.where(x != 0, 1.0, 0.0).astype(BF16)
    ones = jnp.ones((8, width), BF16)
    count = lax.dot_general(ones, some, (((1,), (1,)), ((), ())), preferred_element_type=F32)
    valid = count > 0.0
    before = lax.broadcasted_iota(jnp.int32, (slots, slots), 0) < lax.broadcasted_iota(jnp.int32, (slots, slots), 1)
    upper = jnp.where(before, 1.0, 0.0).astype(BF16)
    rank = jnp.dot(jnp.where(valid, 1.0, 0.0).astype(BF16), upper, preferred_element_type=F32)
    rank = jnp.where(valid, rank, -1.0).astype(jnp.int32)
    rows = lax.broadcasted_iota(jnp.int32, (ECAP, slots), 0)
    choose = jnp.where(rows == rank[0:1], 1.0, 0.0).astype(BF16)
    picked = jnp.dot(choose, x, preferred_element_type=F32).astype(BF16)

    acc = jnp.zeros((ECAP, width), F32)
    for k in range(steps):
        cg, cu, cd = copies(go_ref, uo_ref, do_ref, k)
        cg.wait()
        cu.wait()
        if k + ahead < steps:
            fetch(k + ahead)
        gate = jnp.dot(picked, gbuf[k], preferred_element_type=F32)
        up = jnp.dot(picked, ubuf[k], preferred_element_type=F32)
        inner = (jax.nn.gelu(gate, approximate=True) * up).astype(BF16)
        cd.wait()
        acc = acc + jnp.dot(inner, dbuf[k], preferred_element_type=F32)
    out_ref[...] = lax.dot_general(
        choose, acc.astype(BF16), (((0,), (0,)), ((), ())), preferred_element_type=F32
    ).astype(BF16)


def far(x):
    return pltpu.with_memory_space_constraint(x, pltpu.HBM)


def near(x):
    return pltpu.with_memory_space_constraint(x, pltpu.VMEM)


def expert(layer, sec, arrived, weights):
    slots, width = arrived.shape
    tile = 512
    steps = weights[0].shape[-1] // tile
    return pl.pallas_call(
        functools.partial(expert_kernel, layer, tile, 2),
        out_shape=pltpu.VMEM((slots, width), BF16),
        in_specs=[SMEM, VMEM] + [ANY] * 6,
        out_specs=VMEM,
        scratch_shapes=[
            pltpu.VMEM((steps, width, tile), BF16),
            pltpu.VMEM((steps, width, tile), BF16),
            pltpu.VMEM((steps, tile, width), BF16),
            pltpu.SemaphoreType.DMA((3, steps)),
        ],
        compiler_params=pltpu.CompilerParams(vmem_limit_bytes=32 * 2**20),
        name="expert%d" % layer,
    )(sec, near(arrived), *weights)


def small(kernel, outs, *args, name):
    return pl.pallas_call(
        kernel,
        out_shape=[pltpu.VMEM(s, BF16) for s in outs],
        in_specs=[SMEM] + [VMEM] * (len(args) - 1),
        out_specs=[VMEM] * len(outs),
        compiler_params=pltpu.CompilerParams(vmem_limit_bytes=8 * 2**20),
        name=name,
    )(*args)


def on_device(tokens, expert_ids, slots, gates, gain, w_gate, w_up, w_down):
    tok, width = tokens.shape[1:]
    count = lax.axis_size("node") * lax.axis_size("local")
    rows = count * CAP
    axes = ("node", "local")
    sec = lax.axis_index("section").astype(jnp.int32).reshape(1)

    def swap(x):
        return lax.ppermute(x, "section", [(0, 1), (1, 0)])

    def flat(x):
        return x.transpose(0, 1, 3, 2)

    ids_p, slots_p, gain_p, gates_p = swap(expert_ids), swap(slots), swap(gain), swap(gates)
    where = (flat(expert_ids), flat(ids_p), flat(slots), flat(slots_p))
    weight = (flat(gates), flat(gates_p))
    gains = (gain, gain_p)
    own = (w_gate, w_up, w_down)
    sent, _ = lax.optimization_barrier((own, (ids_p, slots_p, gain_p, gates_p)))
    other = tuple(swap(w) for w in sent)

    both = [far(w) for w in own + other]

    def exchange(x):
        x = x.reshape(count, CAP, width)
        return lax.all_to_all(x, axes, split_axis=0, concat_axis=0, tiled=True).reshape(rows, width)

    (packed,) = small(first_kernel, [(rows, width)], sec, tokens, *where, *gains, name="first")
    back = exchange(expert(0, sec, exchange(packed), both))
    h0, packed = small(middle_kernel, [(tok, width), (rows, width)], sec, tokens, near(back), *where, *gains, *weight,
                       name="middle")
    back = exchange(expert(1, sec, exchange(packed), both))
    keep, send = small(last_kernel, [(tok, width), (tok, width)], sec, near(h0), near(back), *where, *weight, name="last")
    got = swap(send)
    first = sec[0] == 0
    return jnp.stack([jnp.where(first, keep, got), jnp.where(first, got, keep)])[None]


def solution(mesh):
    placed = (
        P(None, ("node", "local"), None),
        P("section", None, ("node", "local"), None),
        P("section", None, ("node", "local"), None),
        P("section", None, ("node", "local"), None),
        P("section", None),
        P("section", ("node", "local"), None, None),
        P("section", ("node", "local"), None, None),
        P("section", ("node", "local"), None, None),
    )
    return jax.shard_map(
        on_device,
        mesh=mesh,
        in_specs=placed,
        out_specs=P("section", None, ("node", "local"), None),
        check_vma=False,
    )
```

```python
import functools

import jax
import jax.numpy as jnp
from jax import lax
from jax.experimental import pallas as pl
from jax.experimental.pallas import tpu as pltpu
from jax.sharding import PartitionSpec as P


CAP = 8
ECAP = 256
AHEAD = 3
F32 = jnp.float32
BF16 = jnp.bfloat16
VMEM = pl.BlockSpec(memory_space=pltpu.VMEM)
SMEM = pl.BlockSpec(memory_space=pltpu.SMEM)
ANY = pl.BlockSpec(memory_space=pl.ANY)


def normed_rows(h, gain):
    x = h.astype(F32)
    ms = jnp.mean(x * x, axis=-1, keepdims=True)
    return (x * lax.rsqrt(ms + 1e-05) * gain).astype(BF16)


def pick(sec, layer, own_ref, oth_ref):
    return jnp.where(sec == layer, own_ref[0, sec], oth_ref[0, sec])


def places(sec, layer, ids_ref, idp_ref, slot_ref, slotp_ref):
    slot = pick(sec, layer, slot_ref, slotp_ref)
    return jnp.where(slot >= 0, pick(sec, layer, ids_ref, idp_ref) * CAP + slot, -1)


def pack_rows(normed, pos, slots):
    span = lax.broadcasted_iota(jnp.int32, (slots, normed.shape[0]), 0)
    hit = (span == pos[0:1]) | (span == pos[1:2])
    onehot = jnp.where(hit, 1.0, 0.0).astype(BF16)
    return jnp.dot(onehot, normed, preferred_element_type=F32).astype(BF16)


def mix_rows(h, ret, pos, weight):
    span = lax.broadcasted_iota(jnp.int32, (ret.shape[0], h.shape[0]), 0)
    comb = jnp.where(span == pos[0:1], weight[0:1], 0.0) + jnp.where(span == pos[1:2], weight[1:2], 0.0)
    high = comb.astype(BF16)
    low = (comb - high.astype(F32)).astype(BF16)
    down = (((0,), (0,)), ((), ()))
    mixed = lax.dot_general(high, ret, down, preferred_element_type=F32)
    mixed = mixed + lax.dot_general(low, ret, down, preferred_element_type=F32)
    return (h.astype(F32) + mixed).astype(BF16)


def first_kernel(sec_ref, tok_hbm, ids_hbm, slot_hbm, gain_hbm, idp_ref, slotp_ref, goth_ref, out_ref,
                 tok_ref, ids_ref, slot_ref, gown_ref, sems):
    sec = sec_ref[0]
    moves = (
        pltpu.make_async_copy(tok_hbm.at[sec], tok_ref, sems.at[0]),
        pltpu.make_async_copy(ids_hbm, ids_ref, sems.at[1]),
        pltpu.make_async_copy(slot_hbm, slot_ref, sems.at[2]),
        pltpu.make_async_copy(gain_hbm, gown_ref, sems.at[3]),
    )
    for m in moves:
        m.start()
    for m in moves:
        m.wait()
    gain = jnp.where(sec == 0, gown_ref[...], goth_ref[...])
    pos = places(sec, 0, ids_ref, idp_ref, slot_ref, slotp_ref)
    out_ref[...] = pack_rows(normed_rows(tok_ref[...], gain), pos, out_ref.shape[0])


def first(sec, tokens, ids, slot, gain, ids_p, slot_p, gain_p, rows):
    width = tokens.shape[-1]
    return pl.pallas_call(
        first_kernel,
        out_shape=pltpu.VMEM((rows, width), BF16),
        in_specs=[SMEM] + [ANY] * 4 + [VMEM] * 3,
        out_specs=VMEM,
        scratch_shapes=[
            pltpu.VMEM(tokens.shape[1:], BF16),
            pltpu.VMEM(ids.shape, ids.dtype),
            pltpu.VMEM(slot.shape, slot.dtype),
            pltpu.VMEM(gain.shape, gain.dtype),
            pltpu.SemaphoreType.DMA((4,)),
        ],
        compiler_params=pltpu.CompilerParams(vmem_limit_bytes=8 * 2**20),
        name="first",
    )(sec, far(tokens), far(ids), far(slot), far(gain), near(ids_p), near(slot_p), near(gain_p))


def middle_kernel(sec_ref, tok_ref, ret_ref, ids_ref, idp_ref, slot_ref, slotp_ref, gown_ref, goth_ref,
                  wown_ref, woth_ref, h_ref, out_ref):
    sec = sec_ref[0]
    pos = places(sec, 0, ids_ref, idp_ref, slot_ref, slotp_ref)
    h = mix_rows(tok_ref[sec], ret_ref[...], pos, pick(sec, 0, wown_ref, woth_ref))
    h_ref[...] = h
    gain = jnp.where(sec == 1, gown_ref[...], goth_ref[...])
    pos = places(sec, 1, ids_ref, idp_ref, slot_ref, slotp_ref)
    out_ref[...] = pack_rows(normed_rows(h, gain), pos, out_ref.shape[0])


def last_kernel(sec_ref, h_ref, ret_ref, ids_ref, idp_ref, slot_ref, slotp_ref, wown_ref, woth_ref, keep_ref, send_ref):
    sec = sec_ref[0]
    h0 = h_ref[...]
    pos = places(sec, 1, ids_ref, idp_ref, slot_ref, slotp_ref)
    h1 = mix_rows(h0, ret_ref[...], pos, pick(sec, 1, wown_ref, woth_ref))
    keep_ref[...] = jnp.where(sec == 0, h0, h1)
    send_ref[...] = jnp.where(sec == 0, h1, h0)


def chooser(x):
    slots, width = x.shape
    some = jnp.where(x != 0, 1.0, 0.0).astype(BF16)
    ones = jnp.ones((8, width), BF16)
    count = lax.dot_general(ones, some, (((1,), (1,)), ((), ())), preferred_element_type=F32)
    valid = count > 0.0
    before = lax.broadcasted_iota(jnp.int32, (slots, slots), 0) < lax.broadcasted_iota(jnp.int32, (slots, slots), 1)
    upper = jnp.where(before, 1.0, 0.0).astype(BF16)
    rank = jnp.dot(jnp.where(valid, 1.0, 0.0).astype(BF16), upper, preferred_element_type=F32)
    rank = jnp.where(valid, rank, -1.0).astype(jnp.int32)
    rows = lax.broadcasted_iota(jnp.int32, (ECAP, slots), 0)
    return jnp.where(rows == rank[0:1], 1.0, 0.0).astype(BF16)


def spread(choose, acc):
    back = lax.dot_general(choose, acc.astype(BF16), (((0,), (0,)), ((), ())), preferred_element_type=F32)
    return back.astype(BF16)


def expert_kernel(layer, tiles, sec_ref, x_ref, go_ref, uo_ref, do_ref, gp_ref, up_ref, dp_ref, out_ref,
                  gbuf, ubuf, dbuf, sems):
    sec = sec_ref[0]

    def copies(g, u, d, k):
        cols = pl.ds(*tiles[k])
        return (
            pltpu.make_async_copy(g.at[0, 0, :, cols], gbuf.at[:, cols], sems.at[0, k]),
            pltpu.make_async_copy(u.at[0, 0, :, cols], ubuf.at[:, cols], sems.at[1, k]),
            pltpu.make_async_copy(d.at[0, 0, cols, :], dbuf.at[cols, :], sems.at[2, k]),
        )

    def fetch(k):
        @pl.when(sec == layer)
        def _():
            for c in copies(go_ref, uo_ref, do_ref, k):
                c.start()

        @pl.when(sec != layer)
        def _():
            for c in copies(gp_ref, up_ref, dp_ref, k):
                c.start()

    for k in range(AHEAD):
        fetch(k)
    x = x_ref[...]
    choose = chooser(x)
    picked = jnp.dot(choose, x, preferred_element_type=F32).astype(BF16)
    acc = jnp.zeros(picked.shape, F32)
    for k in range(len(tiles)):
        for c in copies(go_ref, uo_ref, do_ref, k):
            c.wait()
        if k + AHEAD < len(tiles):
            fetch(k + AHEAD)
        cols = pl.ds(*tiles[k])
        gate = jnp.dot(picked, gbuf[:, cols], preferred_element_type=F32)
        up = jnp.dot(picked, ubuf[:, cols], preferred_element_type=F32)
        inner = (jax.nn.gelu(gate, approximate=True) * up).astype(BF16)
        acc = acc + jnp.dot(inner, dbuf[cols, :], preferred_element_type=F32)
    out_ref[...] = spread(choose, acc)


def tiles_of(hidden):
    tiles, at = [], 0
    for size in (256, 512):
        tiles.append((at, size))
        at += size
    while at < hidden:
        size = min(768, hidden - at)
        tiles.append((at, size))
        at += size
    return tiles


def far(x):
    return pltpu.with_memory_space_constraint(x, pltpu.HBM)


def near(x):
    return pltpu.with_memory_space_constraint(x, pltpu.VMEM)


def expert(layer, sec, arrived, weights):
    slots, width = arrived.shape
    hidden = weights[0].shape[-1]
    tiles = tiles_of(hidden)
    return pl.pallas_call(
        functools.partial(expert_kernel, layer, tiles),
        out_shape=pltpu.VMEM((slots, width), BF16),
        in_specs=[SMEM, VMEM] + [ANY] * 6,
        out_specs=VMEM,
        scratch_shapes=[
            pltpu.VMEM((width, hidden), BF16),
            pltpu.VMEM((width, hidden), BF16),
            pltpu.VMEM((hidden, width), BF16),
            pltpu.SemaphoreType.DMA((3, len(tiles))),
        ],
        compiler_params=pltpu.CompilerParams(vmem_limit_bytes=32 * 2**20),
    )(sec, near(arrived), *weights)


def small(kernel, outs, *args):
    return pl.pallas_call(
        kernel,
        out_shape=[pltpu.VMEM(s, BF16) for s in outs],
        in_specs=[SMEM] + [VMEM] * (len(args) - 1),
        out_specs=[VMEM] * len(outs),
        compiler_params=pltpu.CompilerParams(vmem_limit_bytes=8 * 2**20),
    )(*args)


def on_device(tokens, expert_ids, slots, gates, gain, w_gate, w_up, w_down):
    tok, width = tokens.shape[1:]
    count = lax.axis_size("node") * lax.axis_size("local")
    rows = count * CAP
    axes = ("node", "local")
    sec = lax.axis_index("section").astype(jnp.int32).reshape(1)

    def swap(x):
        return lax.ppermute(x, "section", [(0, 1), (1, 0)])

    def flat(x):
        return x.transpose(0, 1, 3, 2)

    ids_p, slots_p, gain_p = swap(expert_ids), swap(slots), swap(gain)
    gates_p = swap(gates)
    where = (flat(expert_ids), flat(ids_p), flat(slots), flat(slots_p))
    gains = (gain, gain_p)
    own = (w_gate, w_up, w_down)
    other = tuple(swap(w) for w in own)
    other, gates_p = lax.optimization_barrier((other, gates_p))
    weight = (flat(gates), flat(gates_p))
    both = [far(w) for w in own + other]

    def exchange(x):
        x = x.reshape(count, CAP, width)
        return lax.all_to_all(x, axes, split_axis=0, concat_axis=0, tiled=True).reshape(rows, width)

    packed = first(sec, tokens, where[0], where[2], gain, where[1], where[3], gain_p, rows)
    back = exchange(expert(0, sec, exchange(packed), both))
    h0, packed = small(middle_kernel, [(tok, width), (rows, width)], sec, tokens, near(back), *where, *gains, *weight)
    back = exchange(expert(1, sec, exchange(packed), both))
    keep, send = small(last_kernel, [(tok, width), (tok, width)], sec, near(h0), near(back), *where, *weight)
    got = swap(send)
    lead = sec[0] == 0
    return jnp.stack([jnp.where(lead, keep, got), jnp.where(lead, got, keep)])[None]


def solution(mesh):
    placed = (
        P(None, ("node", "local"), None),
        P("section", None, ("node", "local"), None),
        P("section", None, ("node", "local"), None),
        P("section", None, ("node", "local"), None),
        P("section", None),
        P("section", ("node", "local"), None, None),
        P("section", ("node", "local"), None, None),
        P("section", ("node", "local"), None, None),
    )
    return jax.shard_map(
        on_device,
        mesh=mesh,
        in_specs=placed,
        out_specs=P("section", None, ("node", "local"), None),
        check_vma=False,
    )
```

```python
import functools

import jax
import jax.numpy as jnp
from jax import lax
from jax.experimental import pallas as pl
from jax.experimental.pallas import tpu as pltpu
from jax.sharding import PartitionSpec as P


CAP = 8
ECAP = 256
AHEAD = 3
CUTS = (1, 1, 2)
F32 = jnp.float32
BF16 = jnp.bfloat16
VMEM = pl.BlockSpec(memory_space=pltpu.VMEM)
SMEM = pl.BlockSpec(memory_space=pltpu.SMEM)
ANY = pl.BlockSpec(memory_space=pl.ANY)


def normed_rows(h, gain):
    x = h.astype(F32)
    ms = jnp.mean(x * x, axis=-1, keepdims=True)
    return (x * lax.rsqrt(ms + 1e-05) * gain).astype(BF16)


def pick(sec, layer, own_ref, oth_ref):
    return jnp.where(sec == layer, own_ref[0, sec], oth_ref[0, sec])


def places(sec, layer, ids_ref, idp_ref, slot_ref, slotp_ref):
    slot = pick(sec, layer, slot_ref, slotp_ref)
    return jnp.where(slot >= 0, pick(sec, layer, ids_ref, idp_ref) * CAP + slot, -1)


def pack_rows(normed, pos, slots):
    span = lax.broadcasted_iota(jnp.int32, (slots, normed.shape[0]), 0)
    hit = (span == pos[0:1]) | (span == pos[1:2])
    onehot = jnp.where(hit, 1.0, 0.0).astype(BF16)
    return jnp.dot(onehot, normed, preferred_element_type=F32).astype(BF16)


def mix_rows(h, ret, pos, weight):
    span = lax.broadcasted_iota(jnp.int32, (ret.shape[0], h.shape[0]), 0)
    comb = jnp.where(span == pos[0:1], weight[0:1], 0.0) + jnp.where(span == pos[1:2], weight[1:2], 0.0)
    high = comb.astype(BF16)
    low = (comb - high.astype(F32)).astype(BF16)
    down = (((0,), (0,)), ((), ()))
    mixed = lax.dot_general(high, ret, down, preferred_element_type=F32)
    mixed = mixed + lax.dot_general(low, ret, down, preferred_element_type=F32)
    return (h.astype(F32) + mixed).astype(BF16)


def first_kernel(sec_ref, tok_hbm, ids_hbm, slot_hbm, gain_hbm, g_hbm, u_hbm, d_hbm, idp_ref, slotp_ref, goth_ref,
                 gates_ref, out_ref, g_ref, u_ref, d_ref, tok_ref, ids_ref, slot_ref, gown_ref, sems, wsems):
    sec = sec_ref[0]
    moves = (
        pltpu.make_async_copy(tok_hbm.at[sec], tok_ref, sems.at[0]),
        pltpu.make_async_copy(ids_hbm, ids_ref, sems.at[1]),
        pltpu.make_async_copy(slot_hbm, slot_ref, sems.at[2]),
        pltpu.make_async_copy(gain_hbm, gown_ref, sems.at[3]),
    )
    pairs = ((g_hbm, g_ref), (u_hbm, u_ref), (d_hbm, d_ref))
    held = []
    for (src, dst), cuts in zip(pairs, CUTS):
        size = dst.shape[0] // cuts
        for at in range(0, dst.shape[0], size):
            part = pl.ds(at, size)
            held.append(pltpu.make_async_copy(src.at[0, 0, part, :], dst.at[part, :], wsems.at[len(held)]))

    for m in moves:
        m.start()

    @pl.when(sec == 0)
    def _():
        held[0].start()

    for m in moves:
        m.wait()
    gain = jnp.where(sec == 0, gown_ref[...], goth_ref[...])
    pos = places(sec, 0, ids_ref, idp_ref, slot_ref, slotp_ref)
    out_ref[...] = pack_rows(normed_rows(tok_ref[...], gain), pos, out_ref.shape[0])

    @pl.when(sec == 0)
    def _():
        for m, later in zip(held, held[1:] + [None]):
            m.wait()
            if later is not None:
                later.start()


def first(sec, tokens, ids, slot, gain, weights, ids_p, slot_p, gain_p, gates_p, rows):
    width = tokens.shape[-1]
    return pl.pallas_call(
        first_kernel,
        out_shape=[pltpu.VMEM((rows, width), BF16)] + [pltpu.VMEM(w.shape[2:], BF16) for w in weights],
        in_specs=[SMEM] + [ANY] * 7 + [VMEM] * 4,
        out_specs=[VMEM] * 4,
        scratch_shapes=[
            pltpu.VMEM(tokens.shape[1:], BF16),
            pltpu.VMEM(ids.shape, ids.dtype),
            pltpu.VMEM(slot.shape, slot.dtype),
            pltpu.VMEM(gain.shape, gain.dtype),
            pltpu.SemaphoreType.DMA((4,)),
            pltpu.SemaphoreType.DMA((sum(CUTS),)),
        ],
        compiler_params=pltpu.CompilerParams(vmem_limit_bytes=8 * 2**20),
        name="first",
    )(sec, far(tokens), far(ids), far(slot), far(gain), *[far(w) for w in weights],
      near(ids_p), near(slot_p), near(gain_p), near(gates_p))


def middle_kernel(sec_ref, tok_ref, ret_ref, ids_ref, idp_ref, slot_ref, slotp_ref, gown_ref, goth_ref,
                  wown_ref, woth_ref, h_ref, out_ref):
    sec = sec_ref[0]
    pos = places(sec, 0, ids_ref, idp_ref, slot_ref, slotp_ref)
    h = mix_rows(tok_ref[sec], ret_ref[...], pos, pick(sec, 0, wown_ref, woth_ref))
    h_ref[...] = h
    gain = jnp.where(sec == 1, gown_ref[...], goth_ref[...])
    pos = places(sec, 1, ids_ref, idp_ref, slot_ref, slotp_ref)
    out_ref[...] = pack_rows(normed_rows(h, gain), pos, out_ref.shape[0])


def last_kernel(sec_ref, h_ref, ret_ref, ids_ref, idp_ref, slot_ref, slotp_ref, wown_ref, woth_ref, keep_ref, send_ref):
    sec = sec_ref[0]
    h0 = h_ref[...]
    pos = places(sec, 1, ids_ref, idp_ref, slot_ref, slotp_ref)
    h1 = mix_rows(h0, ret_ref[...], pos, pick(sec, 1, wown_ref, woth_ref))
    keep_ref[...] = jnp.where(sec == 0, h0, h1)
    send_ref[...] = jnp.where(sec == 0, h1, h0)


def chooser(x):
    slots, width = x.shape
    some = jnp.where(x != 0, 1.0, 0.0).astype(BF16)
    ones = jnp.ones((8, width), BF16)
    count = lax.dot_general(ones, some, (((1,), (1,)), ((), ())), preferred_element_type=F32)
    valid = count > 0.0
    before = lax.broadcasted_iota(jnp.int32, (slots, slots), 0) < lax.broadcasted_iota(jnp.int32, (slots, slots), 1)
    upper = jnp.where(before, 1.0, 0.0).astype(BF16)
    rank = jnp.dot(jnp.where(valid, 1.0, 0.0).astype(BF16), upper, preferred_element_type=F32)
    rank = jnp.where(valid, rank, -1.0).astype(jnp.int32)
    rows = lax.broadcasted_iota(jnp.int32, (ECAP, slots), 0)
    return jnp.where(rows == rank[0:1], 1.0, 0.0).astype(BF16)


def spread(choose, acc):
    back = lax.dot_general(choose, acc.astype(BF16), (((0,), (0,)), ((), ())), preferred_element_type=F32)
    return back.astype(BF16)


def hidden_part(picked, g, u, d):
    gate = jnp.dot(picked, g, preferred_element_type=F32)
    up = jnp.dot(picked, u, preferred_element_type=F32)
    inner = (jax.nn.gelu(gate, approximate=True) * up).astype(BF16)
    return jnp.dot(inner, d, preferred_element_type=F32)


def expert_kernel(layer, tiles, sec_ref, x_ref, *refs):
    sec = sec_ref[0]
    held, source = refs[0:3], refs[3:6]
    gbuf, ubuf, dbuf, sems = refs[-4:]
    out_ref = refs[6]
    later = ()
    if layer == 0:
        sems, wsems = refs[-5], refs[-4]
        gbuf, ubuf, dbuf = refs[-3:]
        later = tuple(pltpu.make_async_copy(r.at[0, 0], o, wsems.at[i])
                      for i, (r, o) in enumerate(zip(source, refs[7:10])))

    def copies(k):
        cols = pl.ds(*tiles[k])
        g, u, d = source
        return (
            pltpu.make_async_copy(g.at[0, 0, :, cols], gbuf.at[:, cols], sems.at[0, k]),
            pltpu.make_async_copy(u.at[0, 0, :, cols], ubuf.at[:, cols], sems.at[1, k]),
            pltpu.make_async_copy(d.at[0, 0, cols, :], dbuf.at[cols, :], sems.at[2, k]),
        )

    @pl.when(sec == 1)
    def _():
        for k in range(AHEAD):
            for c in copies(k):
                c.start()

    @pl.when(sec == 0)
    def _():
        for c in later:
            c.start()

    x = x_ref[...]
    choose = chooser(x)
    picked = jnp.dot(choose, x, preferred_element_type=F32).astype(BF16)

    @pl.when(sec == 1)
    def _():
        acc = jnp.zeros(picked.shape, F32)
        for k in range(len(tiles)):
            for c in copies(k):
                c.wait()
            if k + AHEAD < len(tiles):
                for c in copies(k + AHEAD):
                    c.start()
            cols = pl.ds(*tiles[k])
            acc = acc + hidden_part(picked, gbuf[:, cols], ubuf[:, cols], dbuf[cols, :])
        out_ref[...] = spread(choose, acc)

    @pl.when(sec == 0)
    def _():
        g_ref, u_ref, d_ref = held
        acc = jnp.zeros(picked.shape, F32)
        for at, size in tiles:
            cols = pl.ds(at, size)
            acc = acc + hidden_part(picked, g_ref[:, cols], u_ref[:, cols], d_ref[cols, :])
        out_ref[...] = spread(choose, acc)
        for c in later:
            c.wait()


def tiles_of(hidden):
    tiles, at = [], 0
    for size in (256, 512):
        tiles.append((at, size))
        at += size
    while at < hidden:
        size = min(768, hidden - at)
        tiles.append((at, size))
        at += size
    return tiles


def far(x):
    return pltpu.with_memory_space_constraint(x, pltpu.HBM)


def near(x):
    return pltpu.with_memory_space_constraint(x, pltpu.VMEM)


def expert(layer, sec, arrived, held, source):
    slots, width = arrived.shape
    hidden = source[0].shape[-1]
    tiles = tiles_of(hidden)
    bufs = [
        pltpu.VMEM((width, hidden), BF16),
        pltpu.VMEM((width, hidden), BF16),
        pltpu.VMEM((hidden, width), BF16),
    ]
    outs = [pltpu.VMEM((slots, width), BF16)]
    scratch = [pltpu.SemaphoreType.DMA((3, len(tiles)))]
    if layer == 0:
        outs += bufs
        scratch = scratch + [pltpu.SemaphoreType.DMA((3,))] + bufs
    else:
        scratch = bufs + scratch
    return pl.pallas_call(
        functools.partial(expert_kernel, layer, tiles),
        out_shape=outs,
        in_specs=[SMEM] + [VMEM] * 4 + [ANY] * 3,
        out_specs=[VMEM] * len(outs),
        scratch_shapes=scratch,
        compiler_params=pltpu.CompilerParams(vmem_limit_bytes=24 * 2**20),
    )(sec, near(arrived), *[near(w) for w in held], *[far(w) for w in source])


def small(kernel, outs, *args):
    return pl.pallas_call(
        kernel,
        out_shape=[pltpu.VMEM(s, BF16) for s in outs],
        in_specs=[SMEM] + [VMEM] * (len(args) - 1),
        out_specs=[VMEM] * len(outs),
        compiler_params=pltpu.CompilerParams(vmem_limit_bytes=8 * 2**20),
    )(*args)


def on_device(tokens, expert_ids, slots, gates, gain, w_gate, w_up, w_down):
    tok, width = tokens.shape[1:]
    count = lax.axis_size("node") * lax.axis_size("local")
    rows = count * CAP
    axes = ("node", "local")
    sec = lax.axis_index("section").astype(jnp.int32).reshape(1)

    def swap(x):
        return lax.ppermute(x, "section", [(0, 1), (1, 0)])

    def flat(x):
        return x.transpose(0, 1, 3, 2)

    ids_p, slots_p, gain_p = swap(expert_ids), swap(slots), swap(gain)
    gates_p = swap(gates)
    where = (flat(expert_ids), flat(ids_p), flat(slots), flat(slots_p))
    gains = (gain, gain_p)
    own = (w_gate, w_up, w_down)
    other = tuple(swap(w) for w in own)
    weight = (flat(gates), flat(gates_p))

    def exchange(x):
        x = x.reshape(count, CAP, width)
        return lax.all_to_all(x, axes, split_axis=0, concat_axis=0, tiled=True).reshape(rows, width)

    packed, *held = first(sec, tokens, where[0], where[2], gain, own, where[1], where[3], gain_p, weight[1], rows)
    answer, *held = expert(0, sec, exchange(packed), held, other)
    back = exchange(answer)
    h0, packed = small(middle_kernel, [(tok, width), (rows, width)], sec, tokens, near(back), *where, *gains, *weight)
    (answer,) = expert(1, sec, exchange(packed), held, own)
    back = exchange(answer)
    keep, send = small(last_kernel, [(tok, width), (tok, width)], sec, near(h0), near(back), *where, *weight)
    got = swap(send)
    lead = sec[0] == 0
    return jnp.stack([jnp.where(lead, keep, got), jnp.where(lead, got, keep)])[None]


def solution(mesh):
    placed = (
        P(None, ("node", "local"), None),
        P("section", None, ("node", "local"), None),
        P("section", None, ("node", "local"), None),
        P("section", None, ("node", "local"), None),
        P("section", None),
        P("section", ("node", "local"), None, None),
        P("section", ("node", "local"), None, None),
        P("section", ("node", "local"), None, None),
    )
    return jax.shard_map(
        on_device,
        mesh=mesh,
        in_specs=placed,
        out_specs=P("section", None, ("node", "local"), None),
        check_vma=False,
    )
```

```python
import functools

import jax
import jax.numpy as jnp
from jax import lax
from jax.experimental import pallas as pl
from jax.experimental.pallas import tpu as pltpu
from jax.sharding import PartitionSpec as P


CAP = 8
ECAP = 256
AHEAD = 3
CUTS = (1, 1, 1)
F32 = jnp.float32
BF16 = jnp.bfloat16
VMEM = pl.BlockSpec(memory_space=pltpu.VMEM)
SMEM = pl.BlockSpec(memory_space=pltpu.SMEM)
ANY = pl.BlockSpec(memory_space=pl.ANY)


def normed_rows(h, gain):
    x = h.astype(F32)
    ms = jnp.mean(x * x, axis=-1, keepdims=True)
    return (x * lax.rsqrt(ms + 1e-05) * gain).astype(BF16)


def pick(sec, layer, own_ref, oth_ref):
    return jnp.where(sec == layer, own_ref[0, sec], oth_ref[0, sec])


def places(sec, layer, ids_ref, idp_ref, slot_ref, slotp_ref):
    slot = pick(sec, layer, slot_ref, slotp_ref)
    return jnp.where(slot >= 0, pick(sec, layer, ids_ref, idp_ref) * CAP + slot, -1)


def pack_rows(normed, pos, slots):
    span = lax.broadcasted_iota(jnp.int32, (slots, normed.shape[0]), 0)
    hit = (span == pos[0:1]) | (span == pos[1:2])
    onehot = jnp.where(hit, 1.0, 0.0).astype(BF16)
    return jnp.dot(onehot, normed, preferred_element_type=F32).astype(BF16)


def mix_rows(h, ret, pos, weight):
    span = lax.broadcasted_iota(jnp.int32, (ret.shape[0], h.shape[0]), 0)
    comb = jnp.where(span == pos[0:1], weight[0:1], 0.0) + jnp.where(span == pos[1:2], weight[1:2], 0.0)
    high = comb.astype(BF16)
    low = (comb - high.astype(F32)).astype(BF16)
    down = (((0,), (0,)), ((), ()))
    mixed = lax.dot_general(high, ret, down, preferred_element_type=F32)
    mixed = mixed + lax.dot_general(low, ret, down, preferred_element_type=F32)
    return (h.astype(F32) + mixed).astype(BF16)


def first_kernel(sec_ref, tok_hbm, ids_hbm, slot_hbm, gain_hbm, g_hbm, u_hbm, d_hbm, idp_ref, slotp_ref, goth_ref,
                 gates_ref, out_ref, g_ref, u_ref, d_ref, tok_ref, ids_ref, slot_ref, gown_ref, sems, wsems):
    sec = sec_ref[0]
    moves = (
        pltpu.make_async_copy(tok_hbm.at[sec], tok_ref, sems.at[0]),
        pltpu.make_async_copy(ids_hbm, ids_ref, sems.at[1]),
        pltpu.make_async_copy(slot_hbm, slot_ref, sems.at[2]),
        pltpu.make_async_copy(gain_hbm, gown_ref, sems.at[3]),
    )
    pairs = ((g_hbm, g_ref), (u_hbm, u_ref), (d_hbm, d_ref))
    held = []
    for (src, dst), cuts in zip(pairs, CUTS):
        size = dst.shape[0] // cuts
        for at in range(0, dst.shape[0], size):
            part = pl.ds(at, size)
            held.append(pltpu.make_async_copy(src.at[0, 0, part, :], dst.at[part, :], wsems.at[len(held)]))

    for m in moves:
        m.start()

    @pl.when(sec == 0)
    def _():
        for m in held:
            m.start()

    for m in moves:
        m.wait()
    gain = jnp.where(sec == 0, gown_ref[...], goth_ref[...])
    pos = places(sec, 0, ids_ref, idp_ref, slot_ref, slotp_ref)
    out_ref[...] = pack_rows(normed_rows(tok_ref[...], gain), pos, out_ref.shape[0])

    @pl.when(sec == 0)
    def _():
        for m in held:
            m.wait()


def first(sec, tokens, ids, slot, gain, weights, ids_p, slot_p, gain_p, gates_p, rows):
    width = tokens.shape[-1]
    return pl.pallas_call(
        first_kernel,
        out_shape=[pltpu.VMEM((rows, width), BF16)] + [pltpu.VMEM(w.shape[2:], BF16) for w in weights],
        in_specs=[SMEM] + [ANY] * 7 + [VMEM] * 4,
        out_specs=[VMEM] * 4,
        scratch_shapes=[
            pltpu.VMEM(tokens.shape[1:], BF16),
            pltpu.VMEM(ids.shape, ids.dtype),
            pltpu.VMEM(slot.shape, slot.dtype),
            pltpu.VMEM(gain.shape, gain.dtype),
            pltpu.SemaphoreType.DMA((4,)),
            pltpu.SemaphoreType.DMA((sum(CUTS),)),
        ],
        compiler_params=pltpu.CompilerParams(vmem_limit_bytes=8 * 2**20),
        name="first",
    )(sec, far(tokens), far(ids), far(slot), far(gain), *[far(w) for w in weights],
      near(ids_p), near(slot_p), near(gain_p), near(gates_p))


def middle_kernel(sec_ref, tok_ref, ret_ref, ids_ref, idp_ref, slot_ref, slotp_ref, gown_ref, goth_ref,
                  wown_ref, woth_ref, h_ref, out_ref):
    sec = sec_ref[0]
    pos = places(sec, 0, ids_ref, idp_ref, slot_ref, slotp_ref)
    h = mix_rows(tok_ref[sec], ret_ref[...], pos, pick(sec, 0, wown_ref, woth_ref))
    h_ref[...] = h
    gain = jnp.where(sec == 1, gown_ref[...], goth_ref[...])
    pos = places(sec, 1, ids_ref, idp_ref, slot_ref, slotp_ref)
    out_ref[...] = pack_rows(normed_rows(h, gain), pos, out_ref.shape[0])


def last_kernel(sec_ref, h_ref, ret_ref, ids_ref, idp_ref, slot_ref, slotp_ref, wown_ref, woth_ref, keep_ref, send_ref):
    sec = sec_ref[0]
    h0 = h_ref[...]
    pos = places(sec, 1, ids_ref, idp_ref, slot_ref, slotp_ref)
    h1 = mix_rows(h0, ret_ref[...], pos, pick(sec, 1, wown_ref, woth_ref))
    keep_ref[...] = jnp.where(sec == 0, h0, h1)
    send_ref[...] = jnp.where(sec == 0, h1, h0)


def chooser(x):
    slots, width = x.shape
    some = jnp.where(x != 0, 1.0, 0.0).astype(BF16)
    ones = jnp.ones((8, width), BF16)
    count = lax.dot_general(ones, some, (((1,), (1,)), ((), ())), preferred_element_type=F32)
    valid = count > 0.0
    before = lax.broadcasted_iota(jnp.int32, (slots, slots), 0) < lax.broadcasted_iota(jnp.int32, (slots, slots), 1)
    upper = jnp.where(before, 1.0, 0.0).astype(BF16)
    rank = jnp.dot(jnp.where(valid, 1.0, 0.0).astype(BF16), upper, preferred_element_type=F32)
    rank = jnp.where(valid, rank, -1.0).astype(jnp.int32)
    rows = lax.broadcasted_iota(jnp.int32, (ECAP, slots), 0)
    return jnp.where(rows == rank[0:1], 1.0, 0.0).astype(BF16)


def spread(choose, acc):
    back = lax.dot_general(choose, acc.astype(BF16), (((0,), (0,)), ((), ())), preferred_element_type=F32)
    return back.astype(BF16)


def hidden_part(picked, g, u):
    gate = jnp.dot(picked, g, preferred_element_type=F32)
    up = jnp.dot(picked, u, preferred_element_type=F32)
    return (jax.nn.gelu(gate, approximate=True) * up).astype(BF16)


def stream(source, bufs, dims, sems, tiles, use):
    def copies(k):
        at, size = tiles[k]
        for i, (src, buf, dim) in enumerate(zip(source, bufs, dims)):
            part = pl.ds(at, size)
            if dim:
                yield pltpu.make_async_copy(src.at[0, 0, :, part], buf.at[:, part], sems.at[i, k])
            else:
                yield pltpu.make_async_copy(src.at[0, 0, part, :], buf.at[part, :], sems.at[i, k])

    def start():
        for k in range(min(AHEAD, len(tiles))):
            for c in copies(k):
                c.start()

    def run():
        for k in range(len(tiles)):
            for c in copies(k):
                c.wait()
            if k + AHEAD < len(tiles):
                for c in copies(k + AHEAD):
                    c.start()
            use(k)

    return start, run


def widen_kernel(tiles, sec_ref, x_ref, gh_ref, uh_ref, gs_ref, us_ref, choose_ref, inner_ref, gbuf, ubuf, sems, wsems):
    sec = sec_ref[0]
    later = (
        pltpu.make_async_copy(gs_ref.at[0, 0], gbuf, wsems.at[0]),
        pltpu.make_async_copy(us_ref.at[0, 0], ubuf, wsems.at[1]),
    )
    picked_box = []

    def use(k):
        cols = pl.ds(*tiles[k])
        inner_ref[:, cols] = hidden_part(picked_box[0], gbuf[:, cols], ubuf[:, cols])

    start, run = stream((gs_ref, us_ref), (gbuf, ubuf), (1, 1), sems, tiles, use)
    pl.when(sec == 1)(start)

    @pl.when(sec == 0)
    def _():
        for c in later:
            c.start()

    x = x_ref[...]
    choose = chooser(x)
    choose_ref[...] = choose
    picked_box.append(jnp.dot(choose, x, preferred_element_type=F32).astype(BF16))
    pl.when(sec == 1)(run)

    @pl.when(sec == 0)
    def _():
        for at, size in tiles:
            cols = pl.ds(at, size)
            inner_ref[:, cols] = hidden_part(picked_box[0], gh_ref[:, cols], uh_ref[:, cols])
        for c in later:
            c.wait()


def narrow_kernel(tiles, sec_ref, choose_ref, inner_ref, dh_ref, ds_ref, out_ref, dbuf, sems, wsems, acc_ref):
    sec = sec_ref[0]
    later = pltpu.make_async_copy(ds_ref.at[0, 0], dbuf, wsems.at[0])

    def use(k):
        cols = pl.ds(*tiles[k])
        part = jnp.dot(inner_ref[:, cols], dbuf[cols, :], preferred_element_type=F32)
        acc_ref[...] = part if k == 0 else acc_ref[...] + part

    start, run = stream((ds_ref,), (dbuf,), (0,), sems, tiles, use)

    @pl.when(sec == 1)
    def _():
        start()
        run()

    @pl.when(sec == 0)
    def _():
        later.start()
        acc_ref[...] = jnp.dot(inner_ref[...], dh_ref[...], preferred_element_type=F32)
        later.wait()

    out_ref[...] = spread(choose_ref[...], acc_ref[...])


def expert_kernel(tiles, sec_ref, x_ref, gh_ref, uh_ref, dh_ref, gs_ref, us_ref, ds_ref, out_ref,
                  gbuf, ubuf, dbuf, acc_ref, sems):
    sec = sec_ref[0]
    picked_box = []

    def use(k):
        cols = pl.ds(*tiles[k])
        inner = hidden_part(picked_box[0], gbuf[:, cols], ubuf[:, cols])
        part = jnp.dot(inner, dbuf[cols, :], preferred_element_type=F32)
        acc_ref[...] = part if k == 0 else acc_ref[...] + part

    start, run = stream((gs_ref, us_ref, ds_ref), (gbuf, ubuf, dbuf), (1, 1, 0), sems, tiles, use)
    pl.when(sec == 1)(start)
    x = x_ref[...]
    choose = chooser(x)
    picked_box.append(jnp.dot(choose, x, preferred_element_type=F32).astype(BF16))
    pl.when(sec == 1)(run)

    @pl.when(sec == 0)
    def _():
        acc = jnp.zeros(picked_box[0].shape, F32)
        for at, size in tiles:
            cols = pl.ds(at, size)
            inner = hidden_part(picked_box[0], gh_ref[:, cols], uh_ref[:, cols])
            acc = acc + jnp.dot(inner, dh_ref[cols, :], preferred_element_type=F32)
        acc_ref[...] = acc

    out_ref[...] = spread(choose, acc_ref[...])


def tiles_of(hidden):
    tiles, at = [], 0
    for size in (256, 512):
        tiles.append((at, size))
        at += size
    while at < hidden:
        size = min(768, hidden - at)
        tiles.append((at, size))
        at += size
    return tiles


def far(x):
    return pltpu.with_memory_space_constraint(x, pltpu.HBM)


def near(x):
    return pltpu.with_memory_space_constraint(x, pltpu.VMEM)


def open_experts(sec, arrived, held, source):
    slots, width = arrived.shape
    hidden = source[0].shape[-1]
    tiles = tiles_of(hidden)
    choose, inner, g, u = pl.pallas_call(
        functools.partial(widen_kernel, tiles),
        out_shape=[pltpu.VMEM(s, BF16) for s in ((ECAP, slots), (ECAP, hidden), (width, hidden), (width, hidden))],
        in_specs=[SMEM] + [VMEM] * 3 + [ANY] * 2,
        out_specs=[VMEM] * 4,
        scratch_shapes=[pltpu.SemaphoreType.DMA((2, len(tiles))), pltpu.SemaphoreType.DMA((2,))],
        compiler_params=pltpu.CompilerParams(vmem_limit_bytes=16 * 2**20),
        name="widen",
    )(sec, near(arrived), near(held[0]), near(held[1]), far(source[0]), far(source[1]))
    parts = [(at, 1024) for at in range(0, hidden, 1024)]
    answer, d = pl.pallas_call(
        functools.partial(narrow_kernel, parts),
        out_shape=[pltpu.VMEM((slots, width), BF16), pltpu.VMEM((hidden, width), BF16)],
        in_specs=[SMEM] + [VMEM] * 3 + [ANY],
        out_specs=[VMEM] * 2,
        scratch_shapes=[
            pltpu.SemaphoreType.DMA((1, len(parts))),
            pltpu.SemaphoreType.DMA((1,)),
            pltpu.VMEM((ECAP, width), F32),
        ],
        compiler_params=pltpu.CompilerParams(vmem_limit_bytes=16 * 2**20),
        name="narrow",
    )(sec, near(choose), near(inner), near(held[2]), far(source[2]))
    return answer, (g, u, d)


def experts(sec, arrived, held, source):
    slots, width = arrived.shape
    hidden = source[0].shape[-1]
    tiles = tiles_of(hidden)
    return pl.pallas_call(
        functools.partial(expert_kernel, tiles),
        out_shape=pltpu.VMEM((slots, width), BF16),
        in_specs=[SMEM] + [VMEM] * 4 + [ANY] * 3,
        out_specs=VMEM,
        scratch_shapes=[
            pltpu.VMEM((width, hidden), BF16),
            pltpu.VMEM((width, hidden), BF16),
            pltpu.VMEM((hidden, width), BF16),
            pltpu.VMEM((ECAP, width), F32),
            pltpu.SemaphoreType.DMA((3, len(tiles))),
        ],
        compiler_params=pltpu.CompilerParams(vmem_limit_bytes=24 * 2**20),
        name="experts",
    )(sec, near(arrived), *[near(w) for w in held], *[far(w) for w in source])


def small(kernel, outs, *args):
    return pl.pallas_call(
        kernel,
        out_shape=[pltpu.VMEM(s, BF16) for s in outs],
        in_specs=[SMEM] + [VMEM] * (len(args) - 1),
        out_specs=[VMEM] * len(outs),
        compiler_params=pltpu.CompilerParams(vmem_limit_bytes=8 * 2**20),
    )(*args)


def on_device(tokens, expert_ids, slots, gates, gain, w_gate, w_up, w_down):
    tok, width = tokens.shape[1:]
    count = lax.axis_size("node") * lax.axis_size("local")
    rows = count * CAP
    axes = ("node", "local")
    sec = lax.axis_index("section").astype(jnp.int32).reshape(1)

    def swap(x):
        return lax.ppermute(x, "section", [(0, 1), (1, 0)])

    def flat(x):
        return x.transpose(0, 1, 3, 2)

    ids_p, slots_p, gain_p = swap(expert_ids), swap(slots), swap(gain)
    gates_p = swap(gates)
    where = (flat(expert_ids), flat(ids_p), flat(slots), flat(slots_p))
    gains = (gain, gain_p)
    own = (w_gate, w_up, w_down)
    other = tuple(swap(w) for w in own)
    weight = (flat(gates), flat(gates_p))

    def exchange(x):
        x = x.reshape(count, CAP, width)
        return lax.all_to_all(x, axes, split_axis=0, concat_axis=0, tiled=True).reshape(rows, width)

    packed, *held = first(sec, tokens, where[0], where[2], gain, own, where[1], where[3], gain_p, weight[1], rows)
    answer, held = open_experts(sec, exchange(packed), held, other)
    back = exchange(answer)
    h0, packed = small(middle_kernel, [(tok, width), (rows, width)], sec, tokens, near(back), *where, *gains, *weight)
    back = exchange(experts(sec, exchange(packed), held, own))
    keep, send = small(last_kernel, [(tok, width), (tok, width)], sec, near(h0), near(back), *where, *weight)
    got = swap(send)
    lead = sec[0] == 0
    return jnp.stack([jnp.where(lead, keep, got), jnp.where(lead, got, keep)])[None]


def solution(mesh):
    placed = (
        P(None, ("node", "local"), None),
        P("section", None, ("node", "local"), None),
        P("section", None, ("node", "local"), None),
        P("section", None, ("node", "local"), None),
        P("section", None),
        P("section", ("node", "local"), None, None),
        P("section", ("node", "local"), None, None),
        P("section", ("node", "local"), None, None),
    )
    return jax.shard_map(
        on_device,
        mesh=mesh,
        in_specs=placed,
        out_specs=P("section", None, ("node", "local"), None),
        check_vma=False,
    )
```

```python
import functools

import jax
import jax.numpy as jnp
from jax import lax
from jax.experimental import pallas as pl
from jax.experimental.pallas import tpu as pltpu
from jax.sharding import PartitionSpec as P


CAP = 8
ECAP = 256
AHEAD = 3
CUTS = (1, 1, 1)
F32 = jnp.float32
BF16 = jnp.bfloat16
VMEM = pl.BlockSpec(memory_space=pltpu.VMEM)
SMEM = pl.BlockSpec(memory_space=pltpu.SMEM)
ANY = pl.BlockSpec(memory_space=pl.ANY)


def normed_rows(h, gain):
    x = h.astype(F32)
    ms = jnp.mean(x * x, axis=-1, keepdims=True)
    return (x * lax.rsqrt(ms + 1e-05) * gain).astype(BF16)


def pick(sec, layer, own_ref, oth_ref):
    return jnp.where(sec == layer, own_ref[0, sec], oth_ref[0, sec])


def places(sec, layer, ids_ref, idp_ref, slot_ref, slotp_ref):
    slot = pick(sec, layer, slot_ref, slotp_ref)
    return jnp.where(slot >= 0, pick(sec, layer, ids_ref, idp_ref) * CAP + slot, -1)


def pack_rows(normed, pos, slots):
    span = lax.broadcasted_iota(jnp.int32, (slots, normed.shape[0]), 0)
    hit = (span == pos[0:1]) | (span == pos[1:2])
    onehot = jnp.where(hit, 1.0, 0.0).astype(BF16)
    return jnp.dot(onehot, normed, preferred_element_type=F32).astype(BF16)


def mix_rows(h, ret, pos, weight):
    tok = h.shape[0]
    pos = jnp.concatenate([pos, pos], axis=1)
    weight = jnp.concatenate([weight, weight], axis=1)
    shape = (ret.shape[0], 2 * tok)
    span = lax.broadcasted_iota(jnp.int32, shape, 0)
    comb = jnp.where(span == pos[0:1], weight[0:1], 0.0) + jnp.where(span == pos[1:2], weight[1:2], 0.0)
    high = comb.astype(BF16).astype(F32)
    left = lax.broadcasted_iota(jnp.int32, shape, 1) < tok
    both = jnp.where(left, high, comb - high).astype(BF16)
    mixed = lax.dot_general(both, ret, (((0,), (0,)), ((), ())), preferred_element_type=F32)
    return (h.astype(F32) + (mixed[:tok] + mixed[tok:])).astype(BF16)


def first_kernel(sec_ref, tok_hbm, ids_hbm, slot_hbm, gain_hbm, g_hbm, u_hbm, d_hbm, idp_ref, slotp_ref, goth_ref,
                 gates_ref, out_ref, g_ref, u_ref, d_ref, tok_ref, ids_ref, slot_ref, gown_ref, sems, wsems):
    sec = sec_ref[0]
    moves = (
        pltpu.make_async_copy(tok_hbm.at[sec], tok_ref, sems.at[0]),
        pltpu.make_async_copy(ids_hbm, ids_ref, sems.at[1]),
        pltpu.make_async_copy(slot_hbm, slot_ref, sems.at[2]),
        pltpu.make_async_copy(gain_hbm, gown_ref, sems.at[3]),
    )
    pairs = ((g_hbm, g_ref), (u_hbm, u_ref), (d_hbm, d_ref))
    held = []
    for (src, dst), cuts in zip(pairs, CUTS):
        size = dst.shape[0] // cuts
        for at in range(0, dst.shape[0], size):
            part = pl.ds(at, size)
            held.append(pltpu.make_async_copy(src.at[0, 0, part, :], dst.at[part, :], wsems.at[len(held)]))

    for m in moves:
        m.start()

    @pl.when(sec == 0)
    def _():
        for m in held:
            m.start()

    for m in moves:
        m.wait()
    gain = jnp.where(sec == 0, gown_ref[...], goth_ref[...])
    pos = places(sec, 0, ids_ref, idp_ref, slot_ref, slotp_ref)
    out_ref[...] = pack_rows(normed_rows(tok_ref[...], gain), pos, out_ref.shape[0])

    @pl.when(sec == 0)
    def _():
        for m in held:
            m.wait()


def first(sec, tokens, ids, slot, gain, weights, ids_p, slot_p, gain_p, gates_p, rows):
    width = tokens.shape[-1]
    return pl.pallas_call(
        first_kernel,
        out_shape=[pltpu.VMEM((rows, width), BF16)] + [pltpu.VMEM(w.shape[2:], BF16) for w in weights],
        in_specs=[SMEM] + [ANY] * 7 + [VMEM] * 4,
        out_specs=[VMEM] * 4,
        scratch_shapes=[
            pltpu.VMEM(tokens.shape[1:], BF16),
            pltpu.VMEM(ids.shape, ids.dtype),
            pltpu.VMEM(slot.shape, slot.dtype),
            pltpu.VMEM(gain.shape, gain.dtype),
            pltpu.SemaphoreType.DMA((4,)),
            pltpu.SemaphoreType.DMA((sum(CUTS),)),
        ],
        compiler_params=pltpu.CompilerParams(vmem_limit_bytes=8 * 2**20),
        name="first",
    )(sec, far(tokens), far(ids), far(slot), far(gain), *[far(w) for w in weights],
      near(ids_p), near(slot_p), near(gain_p), near(gates_p))


def middle_kernel(sec_ref, tok_ref, ret_ref, ids_ref, idp_ref, slot_ref, slotp_ref, gown_ref, goth_ref,
                  wown_ref, woth_ref, h_ref, out_ref):
    sec = sec_ref[0]
    pos = places(sec, 0, ids_ref, idp_ref, slot_ref, slotp_ref)
    h = mix_rows(tok_ref[sec], ret_ref[...], pos, pick(sec, 0, wown_ref, woth_ref))
    h_ref[...] = h
    gain = jnp.where(sec == 1, gown_ref[...], goth_ref[...])
    pos = places(sec, 1, ids_ref, idp_ref, slot_ref, slotp_ref)
    out_ref[...] = pack_rows(normed_rows(h, gain), pos, out_ref.shape[0])


def last_kernel(sec_ref, h_ref, ret_ref, ids_ref, idp_ref, slot_ref, slotp_ref, wown_ref, woth_ref, keep_ref, send_ref):
    sec = sec_ref[0]
    h0 = h_ref[...]
    pos = places(sec, 1, ids_ref, idp_ref, slot_ref, slotp_ref)
    h1 = mix_rows(h0, ret_ref[...], pos, pick(sec, 1, wown_ref, woth_ref))
    keep_ref[...] = jnp.where(sec == 0, h0, h1)
    send_ref[...] = jnp.where(sec == 0, h1, h0)


def chooser(x):
    slots, width = x.shape
    some = jnp.where(x != 0, 1.0, 0.0).astype(BF16)
    ones = jnp.ones((8, width), BF16)
    count = lax.dot_general(ones, some, (((1,), (1,)), ((), ())), preferred_element_type=F32)
    valid = count > 0.0
    before = lax.broadcasted_iota(jnp.int32, (slots, slots), 0) < lax.broadcasted_iota(jnp.int32, (slots, slots), 1)
    upper = jnp.where(before, 1.0, 0.0).astype(BF16)
    rank = jnp.dot(jnp.where(valid, 1.0, 0.0).astype(BF16), upper, preferred_element_type=F32)
    rank = jnp.where(valid, rank, -1.0).astype(jnp.int32)
    rows = lax.broadcasted_iota(jnp.int32, (ECAP, slots), 0)
    return jnp.where(rows == rank[0:1], 1.0, 0.0).astype(BF16)


def spread(choose, acc):
    back = lax.dot_general(choose, acc.astype(BF16), (((0,), (0,)), ((), ())), preferred_element_type=F32)
    return back.astype(BF16)


def hidden_part(picked, g, u):
    gate = jnp.dot(picked, g, preferred_element_type=F32)
    up = jnp.dot(picked, u, preferred_element_type=F32)
    return (jax.nn.gelu(gate, approximate=True) * up).astype(BF16)


def stream(source, bufs, dims, sems, tiles, use):
    def copies(k):
        at, size = tiles[k]
        for i, (src, buf, dim) in enumerate(zip(source, bufs, dims)):
            part = pl.ds(at, size)
            if dim:
                yield pltpu.make_async_copy(src.at[0, 0, :, part], buf.at[:, part], sems.at[i, k])
            else:
                yield pltpu.make_async_copy(src.at[0, 0, part, :], buf.at[part, :], sems.at[i, k])

    def start():
        for k in range(min(AHEAD, len(tiles))):
            for c in copies(k):
                c.start()

    def run():
        for k in range(len(tiles)):
            for c in copies(k):
                c.wait()
            if k + AHEAD < len(tiles):
                for c in copies(k + AHEAD):
                    c.start()
            use(k)

    return start, run


def widen_kernel(tiles, sec_ref, x_ref, gh_ref, uh_ref, gs_ref, us_ref, choose_ref, inner_ref, gbuf, ubuf, sems, wsems):
    sec = sec_ref[0]
    later = (
        pltpu.make_async_copy(gs_ref.at[0, 0], gbuf, wsems.at[0]),
        pltpu.make_async_copy(us_ref.at[0, 0], ubuf, wsems.at[1]),
    )
    picked_box = []

    def use(k):
        cols = pl.ds(*tiles[k])
        inner_ref[:, cols] = hidden_part(picked_box[0], gbuf[:, cols], ubuf[:, cols])

    start, run = stream((gs_ref, us_ref), (gbuf, ubuf), (1, 1), sems, tiles, use)
    pl.when(sec == 1)(start)

    @pl.when(sec == 0)
    def _():
        for c in later:
            c.start()

    x = x_ref[...]
    choose = chooser(x)
    choose_ref[...] = choose
    picked_box.append(jnp.dot(choose, x, preferred_element_type=F32).astype(BF16))
    pl.when(sec == 1)(run)

    @pl.when(sec == 0)
    def _():
        for at, size in tiles:
            cols = pl.ds(at, size)
            inner_ref[:, cols] = hidden_part(picked_box[0], gh_ref[:, cols], uh_ref[:, cols])
        for c in later:
            c.wait()


def narrow_kernel(tiles, sec_ref, choose_ref, inner_ref, dh_ref, ds_ref, out_ref, dbuf, sems, wsems, acc_ref):
    sec = sec_ref[0]
    later = pltpu.make_async_copy(ds_ref.at[0, 0], dbuf, wsems.at[0])

    def use(k):
        cols = pl.ds(*tiles[k])
        part = jnp.dot(inner_ref[:, cols], dbuf[cols, :], preferred_element_type=F32)
        acc_ref[...] = part if k == 0 else acc_ref[...] + part

    start, run = stream((ds_ref,), (dbuf,), (0,), sems, tiles, use)

    @pl.when(sec == 1)
    def _():
        start()
        run()

    @pl.when(sec == 0)
    def _():
        later.start()
        acc_ref[...] = jnp.dot(inner_ref[...], dh_ref[...], preferred_element_type=F32)
        later.wait()

    out_ref[...] = spread(choose_ref[...], acc_ref[...])


def expert_kernel(tiles, sec_ref, x_ref, gh_ref, uh_ref, dh_ref, gs_ref, us_ref, ds_ref, out_ref,
                  gbuf, ubuf, dbuf, acc_ref, sems):
    sec = sec_ref[0]
    picked_box = []

    def use(k):
        cols = pl.ds(*tiles[k])
        inner = hidden_part(picked_box[0], gbuf[:, cols], ubuf[:, cols])
        part = jnp.dot(inner, dbuf[cols, :], preferred_element_type=F32)
        acc_ref[...] = part if k == 0 else acc_ref[...] + part

    start, run = stream((gs_ref, us_ref, ds_ref), (gbuf, ubuf, dbuf), (1, 1, 0), sems, tiles, use)
    pl.when(sec == 1)(start)
    x = x_ref[...]
    choose = chooser(x)
    picked_box.append(jnp.dot(choose, x, preferred_element_type=F32).astype(BF16))
    pl.when(sec == 1)(run)

    @pl.when(sec == 0)
    def _():
        acc = jnp.zeros(picked_box[0].shape, F32)
        for at, size in tiles:
            cols = pl.ds(at, size)
            inner = hidden_part(picked_box[0], gh_ref[:, cols], uh_ref[:, cols])
            acc = acc + jnp.dot(inner, dh_ref[cols, :], preferred_element_type=F32)
        acc_ref[...] = acc

    out_ref[...] = spread(choose, acc_ref[...])


def tiles_of(hidden):
    tiles, at = [], 0
    for size in (256, 512):
        tiles.append((at, size))
        at += size
    while at < hidden:
        size = min(768, hidden - at)
        tiles.append((at, size))
        at += size
    return tiles


def far(x):
    return pltpu.with_memory_space_constraint(x, pltpu.HBM)


def near(x):
    return pltpu.with_memory_space_constraint(x, pltpu.VMEM)


def open_experts(sec, arrived, held, source):
    slots, width = arrived.shape
    hidden = source[0].shape[-1]
    tiles = tiles_of(hidden)
    choose, inner, g, u = pl.pallas_call(
        functools.partial(widen_kernel, tiles),
        out_shape=[pltpu.VMEM(s, BF16) for s in ((ECAP, slots), (ECAP, hidden), (width, hidden), (width, hidden))],
        in_specs=[SMEM] + [VMEM] * 3 + [ANY] * 2,
        out_specs=[VMEM] * 4,
        scratch_shapes=[pltpu.SemaphoreType.DMA((2, len(tiles))), pltpu.SemaphoreType.DMA((2,))],
        compiler_params=pltpu.CompilerParams(vmem_limit_bytes=16 * 2**20),
        name="widen",
    )(sec, near(arrived), near(held[0]), near(held[1]), far(source[0]), far(source[1]))
    parts = [(at, 1024) for at in range(0, hidden, 1024)]
    answer, d = pl.pallas_call(
        functools.partial(narrow_kernel, parts),
        out_shape=[pltpu.VMEM((slots, width), BF16), pltpu.VMEM((hidden, width), BF16)],
        in_specs=[SMEM] + [VMEM] * 3 + [ANY],
        out_specs=[VMEM] * 2,
        scratch_shapes=[
            pltpu.SemaphoreType.DMA((1, len(parts))),
            pltpu.SemaphoreType.DMA((1,)),
            pltpu.VMEM((ECAP, width), F32),
        ],
        compiler_params=pltpu.CompilerParams(vmem_limit_bytes=16 * 2**20),
        name="narrow",
    )(sec, near(choose), near(inner), near(held[2]), far(source[2]))
    return answer, (g, u, d)


def experts(sec, arrived, held, source):
    slots, width = arrived.shape
    hidden = source[0].shape[-1]
    tiles = tiles_of(hidden)
    return pl.pallas_call(
        functools.partial(expert_kernel, tiles),
        out_shape=pltpu.VMEM((slots, width), BF16),
        in_specs=[SMEM] + [VMEM] * 4 + [ANY] * 3,
        out_specs=VMEM,
        scratch_shapes=[
            pltpu.VMEM((width, hidden), BF16),
            pltpu.VMEM((width, hidden), BF16),
            pltpu.VMEM((hidden, width), BF16),
            pltpu.VMEM((ECAP, width), F32),
            pltpu.SemaphoreType.DMA((3, len(tiles))),
        ],
        compiler_params=pltpu.CompilerParams(vmem_limit_bytes=24 * 2**20),
        name="experts",
    )(sec, near(arrived), *[near(w) for w in held], *[far(w) for w in source])


def small(kernel, outs, *args):
    return pl.pallas_call(
        kernel,
        out_shape=[pltpu.VMEM(s, BF16) for s in outs],
        in_specs=[SMEM] + [VMEM] * (len(args) - 1),
        out_specs=[VMEM] * len(outs),
        compiler_params=pltpu.CompilerParams(vmem_limit_bytes=8 * 2**20),
    )(*args)


def on_device(tokens, expert_ids, slots, gates, gain, w_gate, w_up, w_down):
    tok, width = tokens.shape[1:]
    count = lax.axis_size("node") * lax.axis_size("local")
    rows = count * CAP
    axes = ("node", "local")
    sec = lax.axis_index("section").astype(jnp.int32).reshape(1)

    def swap(x):
        return lax.ppermute(x, "section", [(0, 1), (1, 0)])

    def flat(x):
        return x.transpose(0, 1, 3, 2)

    ids_p, slots_p, gain_p = swap(expert_ids), swap(slots), swap(gain)
    gates_p = swap(gates)
    where = (flat(expert_ids), flat(ids_p), flat(slots), flat(slots_p))
    gains = (gain, gain_p)
    own = (w_gate, w_up, w_down)
    other = tuple(swap(w) for w in own)
    weight = (flat(gates), flat(gates_p))

    def exchange(x):
        x = x.reshape(count, CAP, width)
        return lax.all_to_all(x, axes, split_axis=0, concat_axis=0, tiled=True).reshape(rows, width)

    packed, *held = first(sec, tokens, where[0], where[2], gain, own, where[1], where[3], gain_p, weight[1], rows)
    answer, held = open_experts(sec, exchange(packed), held, other)
    back = exchange(answer)
    h0, packed = small(middle_kernel, [(tok, width), (rows, width)], sec, tokens, near(back), *where, *gains, *weight)
    back = exchange(experts(sec, exchange(packed), held, own))
    keep, send = small(last_kernel, [(tok, width), (tok, width)], sec, near(h0), near(back), *where, *weight)
    got = swap(send)
    lead = sec[0] == 0
    return jnp.stack([jnp.where(lead, keep, got), jnp.where(lead, got, keep)])[None]


def solution(mesh):
    placed = (
        P(None, ("node", "local"), None),
        P("section", None, ("node", "local"), None),
        P("section", None, ("node", "local"), None),
        P("section", None, ("node", "local"), None),
        P("section", None),
        P("section", ("node", "local"), None, None),
        P("section", ("node", "local"), None, None),
        P("section", ("node", "local"), None, None),
    )
    return jax.shard_map(
        on_device,
        mesh=mesh,
        in_specs=placed,
        out_specs=P("section", None, ("node", "local"), None),
        check_vma=False,
    )
```
